32 devices in a mesh: dp: 16 (over z, y, x), mp: 2 (over core).
Axes of the slice: x: 2, y: 2, z: 4, core: 2. Of those that a mesh axis runs over, the one named last changes fastest.
Arguments:
- points: bfloat16 [16384, 1024], P(('dp', 'mp')), may hold values from -6 to 6
- centroids: bfloat16 [4096, 1024], P('mp'), may hold values from -6 to 6
- assign: int32 [16384], P(('dp', 'mp')), may hold values from 0 to 4095
- keep_mask: int32 [16384], P(('dp', 'mp')), may hold values 0 or 1
Outputs:
- new_centroids: float32 [4096, 1024], P('mp')
- row_cost: float32 [16384], P(('dp', 'mp'))
The draws below stay inside these ranges and needn't reach their ends.
All inputs are finite; a program needn't handle non-finite values. No bound on the sum of `keep_mask` on one device may be relied on, other than what follows from the above.
Results may differ from the reference program's by a relative error of at most 0.0008.
Values may be sent and summed in bfloat16 or wider, within the bound.
No kernel may reach another device: no remote copies, remote signals or barrier semaphores. Data moves between devices by JAX's collectives and lax.ppermute only.
A program may use at most 128 MiB of HBM per device.

```python
import math
import jax
import jax.numpy as jnp
import numpy as np
from jax import lax

D = 1024
K = 4096
ROWS = 16384


def place_ends(values, stream_key, smallest, high):
    longest = values.shape.index(max(values.shape))
    spots = []
    for shift in (0, 1):
        where = [jax.random.randint(jax.random.fold_in(stream_key, axis), (), 0, length) for axis, length in enumerate(values.shape)]
        where[longest] = (where[longest] + shift) % values.shape[longest]
        spots.append(tuple(where))
    return values.at[spots[0]].set(smallest).at[spots[1]].set(high)


def block_scale(own_key, dims, shards, smallest, high):
    level = 1.0
    for axis_at, shards_of in shards:
        draws = jax.random.uniform(jax.random.fold_in(jax.random.fold_in(own_key, 6), axis_at), (shards_of,), jnp.float32, smallest / len(shards), high / len(shards))
        level = level * jnp.repeat(jnp.exp(draws), dims[axis_at] // shards_of).reshape((-1,) + (1,) * (len(dims) - 1 - axis_at))
    return level


def cumulative_ranks(count, lean):
    portions = [(1 << 20) // math.isqrt(standing ** lean) + 1 for standing in range(1, count + 1)]
    width = 1 + sum(portions) // (1 << 30)
    return np.cumsum(np.array([max(1, weight // width) for weight in portions]))


def skewed_ids(own_key, extent, count, skew):
    grid = cumulative_ranks(count, skew)
    pick = jax.random.randint(jax.random.fold_in(own_key, 1), extent, 0, int(grid[count - 1]))
    standing = jnp.searchsorted(jnp.asarray(grid, jnp.int32), pick, side="right")
    return jax.random.permutation(jax.random.fold_in(own_key, 2), count)[standing].astype(jnp.int32)


def centred(own_key, shape, deviation, limit, cuts=(), kind=jnp.bfloat16):
    result = deviation * jax.random.normal(own_key, shape, jnp.float32)
    if cuts:
        result = result * block_scale(own_key, shape, cuts, -0.22, 0.18)
    return jnp.clip(result, -limit, limit).astype(kind)


def setup_inputs(seed: int = 0) -> dict:
    seeds = jax.random.split(jax.random.key(seed), 5)
    points = centred(seeds[0], (ROWS, D), 1.0, 6.0, ((0, 32),))
    centroids = centred(seeds[1], (K, D), 1.0, 6.0, ((0, 2),))
    assign = place_ends(skewed_ids(seeds[2], (ROWS,), K, 2), jax.random.fold_in(seeds[2], 3), 0, K - 1).astype(jnp.int32)
    keep_mask = place_ends((jax.random.randint(seeds[3], (ROWS,), 0, 4) < 3).astype(jnp.int32), jax.random.fold_in(seeds[3], 1), 0, 1)
    return dict(points=points, centroids=centroids, assign=assign, keep_mask=keep_mask)


def reference(points, centroids, assign, keep_mask):
    cent_f = centroids.astype(jnp.float32)
    cent_sq = jnp.sum(cent_f * cent_f, axis=1)
    block = math.gcd(ROWS, 1024)
    blocks = points.reshape(ROWS // block, block, D)

    def cost_block(group_rows):
        point_f = group_rows.astype(jnp.float32)
        point_sq = jnp.sum(point_f * point_f, axis=1)
        inner = jnp.dot(group_rows, centroids.T, preferred_element_type=jnp.float32)
        dist = point_sq[:, None] - 2.0 * inner + cent_sq[None, :]
        return jnp.min(dist, axis=1) / D

    row_cost = lax.map(cost_block, blocks).reshape(ROWS)
    weights = keep_mask.astype(jnp.float32)
    sums = jax.ops.segment_sum(points.astype(jnp.float32) * weights[:, None], assign, num_segments=K)
    counts = jax.ops.segment_sum(weights, assign, num_segments=K)
    fresh = sums / jnp.maximum(counts, 1.0)[:, None]
    new_centroids = jnp.where(counts[:, None] > 0.5, fresh, cent_f)
    return new_centroids, row_cost
```

```python
import functools

import jax
import jax.numpy as jnp
from jax import lax
from jax.experimental import pallas as pl
from jax.experimental.pallas import tpu as pltpu
from jax.sharding import Mesh, PartitionSpec as P

LANES = 128
COLS = 64
LOW = 4
DIGIT = 7
CODE_ROWS = 16
LEVELS = 32767.0
TINY = 1e-30
F32, BF16, I32 = jnp.float32, jnp.bfloat16, jnp.int32
HALF = LANES // 2
SWAP = [(0, 1), (1, 0)]
OWNERS = ("z", "y", "x")
AXES = ("g",) + OWNERS + ("mp",)

VMEM = pl.BlockSpec(memory_space=pltpu.VMEM)
SMEM = pl.BlockSpec(memory_space=pltpu.SMEM)


def pack_kernel(points_ref, assign_ref, keep_ref, out_ref):
    rows, width = points_ref.shape
    blocks = rows // LANES
    kept = keep_ref[...]
    assign = assign_ref[...]
    high = jnp.where(kept > 0, assign >> DIGIT, -1).astype(F32)
    low = (assign & ((1 << DIGIT) - 1)).astype(F32)
    weight = kept.astype(F32)
    peak = jnp.zeros((1, LANES), F32)
    for b in range(blocks):
        for c in range(width // LANES):
            tile = points_ref[b * LANES : (b + 1) * LANES, c * LANES : (c + 1) * LANES].T
            out_ref[2 * c, b * COLS : (b + 1) * COLS, :] = tile[:COLS]
            out_ref[2 * c + 1, b * COLS : (b + 1) * COLS, :] = tile[COLS:]
            size = jnp.max(jnp.abs(tile.astype(F32)), axis=0, keepdims=True)
            peak = jnp.maximum(peak, size * weight[b : b + 1])
    pad = jnp.zeros((CODE_ROWS - 2 * blocks - 1, LANES), F32)
    codes = jnp.concatenate([high, low, peak, pad], axis=0).astype(BF16)
    for s in range(out_ref.shape[0]):
        out_ref[s, blocks * COLS :, :] = codes


def pack(points, assign, keep):
    rows, width = points.shape
    blocks = rows // LANES
    assert 2 * blocks + 1 <= CODE_ROWS
    shape = (width // COLS, blocks * COLS + CODE_ROWS, LANES)
    return pl.pallas_call(
        pack_kernel,
        out_shape=jax.ShapeDtypeStruct(shape, BF16),
        in_specs=[VMEM] * 3,
        out_specs=VMEM,
        cost_estimate=pl.CostEstimate(
            flops=2 * rows * width, bytes_accessed=4 * rows * width, transcendentals=0
        ),
        name="pack",
    )(points, assign.reshape(blocks, LANES), keep.reshape(blocks, LANES))


def add_sources(base, recv_ref, acc_ref):
    sources, height, _ = recv_ref.shape
    high_size = acc_ref.shape[1]
    blocks = (height - CODE_ROWS) // COLS
    rows = blocks * LANES
    shift = high_size.bit_length() - 1

    def step(s, peak):
        codes = recv_ref[s, blocks * COLS :, :].astype(F32)
        scale = float(1 << DIGIT)
        digits = [codes[b : b + 1] * scale + codes[blocks + b : blocks + b + 1] for b in range(blocks)]
        local = jnp.concatenate(digits, axis=1).astype(I32) - base
        k_low = local >> shift
        k_high = local & (high_size - 1)
        hot = (lax.broadcasted_iota(I32, (high_size, rows), 0) == k_high).astype(F32).astype(BF16)
        data = [recv_ref[s, b * COLS : (b + 1) * COLS, :] for b in range(blocks)]
        data = jnp.concatenate(data, axis=1)
        masks = [(k_low == l).astype(F32) for l in range(LOW)]
        parts = [data * m.astype(BF16) for m in masks]
        pad = jnp.zeros((CODE_ROWS - LOW, rows), F32)
        parts.append(jnp.concatenate(masks + [pad], axis=0).astype(BF16))
        left = jnp.concatenate(parts, axis=0)
        acc_ref[...] += lax.dot_general(
            left, hot, (((1,), (1,)), ((), ())), preferred_element_type=F32
        )
        return jnp.maximum(peak, codes[2 * blocks : 2 * blocks + 1])

    return lax.fori_loop(0, sources, step, jnp.zeros((1, LANES), F32))


def first_kernel(where_ref, recv_ref, acc_ref, peak_ref):
    acc_ref[...] = jnp.zeros_like(acc_ref)
    peak = add_sources(where_ref[0], recv_ref, acc_ref)
    peak_ref[...] = jnp.broadcast_to(peak, peak_ref.shape)


def second_kernel(where_ref, recv_ref, given_ref, given_peak_ref, acc_ref, peak_ref):
    acc_ref[...] = given_ref[...]
    peak = add_sources(where_ref[0], recv_ref, acc_ref)
    peak_ref[...] = jnp.maximum(given_peak_ref[...], peak)


def sums_of(recv, where, given, high_size):
    sources, height, _ = recv.shape
    rows = (height - CODE_ROWS) // COLS * LANES * sources
    tall = LOW * COLS + CODE_ROWS
    shapes = (jax.ShapeDtypeStruct((tall, high_size), F32), jax.ShapeDtypeStruct((8, LANES), F32))
    cost = pl.CostEstimate(
        flops=2 * rows * tall * high_size, bytes_accessed=recv.size * 2, transcendentals=0
    )
    return pl.pallas_call(
        first_kernel if given is None else second_kernel,
        out_shape=shapes,
        in_specs=[SMEM, VMEM] + ([] if given is None else [VMEM, VMEM]),
        out_specs=(VMEM, VMEM),
        cost_estimate=cost,
        name="sums_first" if given is None else "sums_second",
    )(where, recv, *(given or ()))


def finish_kernel(where_ref, acc_ref, scale_ref, prior_ref, out_ref):
    high_size = acc_ref.shape[1]
    counts = acc_ref[LOW * COLS : LOW * COLS + 8, :]
    inverse = 1.0 / jnp.maximum(counts, 1.0)
    tall = counts.T
    odd = where_ref[1] > 0
    for l in range(LOW):
        mean = acc_ref[l * COLS : (l + 1) * COLS, :] * inverse[l : l + 1]
        prior = prior_ref[l * high_size : (l + 1) * high_size, :].astype(F32)
        prior = jnp.where(odd, pltpu.roll(prior, HALF, 1), prior)[:, :COLS]
        value = jnp.where(tall[:, l : l + 1] > 0.5, mean.T, prior)
        root = jnp.sqrt(jnp.sqrt(jnp.abs(value) * scale_ref[0]))
        level = jnp.minimum(root * LEVELS + 0.5, LEVELS).astype(I32)
        level = jnp.where(value < 0, -level, level).astype(jnp.int16)
        out_ref[:, l * COLS : (l + 1) * COLS] = level


def finish(acc, scale, prior, where):
    high_size = acc.shape[1]
    return pl.pallas_call(
        finish_kernel,
        grid_spec=pltpu.PrefetchScalarGridSpec(
            num_scalar_prefetch=1,
            grid=(1,),
            in_specs=[
                pl.BlockSpec(acc.shape, lambda i, w: (0, 0)),
                SMEM,
                pl.BlockSpec((prior.shape[0], LANES), lambda i, w: (0, w[2])),
            ],
            out_specs=pl.BlockSpec((high_size, LOW * COLS), lambda i, w: (0, 0)),
        ),
        out_shape=jax.ShapeDtypeStruct((high_size, LOW * COLS), jnp.int16),
        cost_estimate=pl.CostEstimate(
            flops=8 * acc.size, bytes_accessed=8 * acc.size, transcendentals=2 * acc.size
        ),
        name="finish",
    )(where, acc, scale, prior)


def spread_kernel(columns_ref, x_ref, peak_ref, mine_ref, other_ref, *refs):
    out_ref = refs[-1]
    high_size = mine_ref.shape[1]
    first = x_ref[0] == 0
    lane = lax.broadcasted_iota(I32, (high_size, LANES), 1)

    def decoded(ref, l):
        t = ref[0, :, l // 2 * LANES : (l // 2 + 1) * LANES].astype(I32).astype(F32) * (1.0 / LEVELS)
        return t * jnp.abs(t) * (t * t) * peak_ref[0]

    for l in range(LOW):
        mine, other = decoded(mine_ref, l), decoded(other_ref, l)
        left, right = jnp.where(first, mine, other), jnp.where(first, other, mine)
        if l % 2:
            left = pltpu.roll(left, HALF, 1)
        else:
            right = pltpu.roll(right, HALF, 1)
        out_ref[l * high_size : (l + 1) * high_size, :] = jnp.where(lane < HALF, left, right)


def spread(mine, other, columns, x, peak, width, into):
    steps, high_size, wide = mine.shape
    total = LOW * high_size
    piece = pl.BlockSpec((1, high_size, wide), lambda i, c: (i, 0, 0))
    extra = [] if into is None else [pl.BlockSpec(memory_space=pl.ANY)]
    return pl.pallas_call(
        spread_kernel,
        grid_spec=pltpu.PrefetchScalarGridSpec(
            num_scalar_prefetch=1,
            grid=(steps,),
            in_specs=[SMEM, SMEM, piece, piece] + extra,
            out_specs=pl.BlockSpec((total, LANES), lambda i, c: (0, c[i])),
        ),
        out_shape=jax.ShapeDtypeStruct((total, width), F32),
        input_output_aliases={} if into is None else {5: 0},
        cost_estimate=pl.CostEstimate(
            flops=8 * steps * total * LANES, bytes_accessed=6 * steps * total * LANES, transcendentals=0
        ),
        name="spread",
    )(columns, x, peak, mine, other, *([] if into is None else [into]))


def nearest(points, point_sq, part):
    inner = lax.dot_general(points, part, (((1,), (1,)), ((), ())), preferred_element_type=F32)
    part_f = part.astype(F32)
    part_sq = jnp.sum(part_f * part_f, axis=1)
    return jnp.min(point_sq[:, None] - 2.0 * inner + part_sq[None, :], axis=1)


def shards(points, centroids, assign, keep_mask):
    width = points.shape[1]
    shard_rows = centroids.shape[0]
    high_size = shard_rows // LOW
    z, y, x = (lax.axis_index(a) for a in OWNERS)
    nz, ny, nx = (lax.axis_size(a) for a in OWNERS)
    assert nx == 2 and ny == 2 and nz * ny * nx * COLS == width
    block = z * ny + y
    where = jnp.stack([lax.axis_index("mp") * shard_rows, x, block]).astype(I32)

    parcels = pack(points, assign, keep_mask)
    recv = lax.all_to_all(parcels, OWNERS, 0, 0, tiled=True)
    partner = lax.ppermute(recv, "mp", SWAP)
    others = lax.ppermute(centroids, "mp", SWAP)

    acc = sums_of(recv, where, None, high_size)
    acc, peak = sums_of(partner, where, acc, high_size)
    peak = jnp.maximum(jnp.max(peak), TINY)
    if lax.axis_size("g") > 1:
        acc, peak = lax.psum(acc, "g"), lax.pmax(peak, "g")
    peak = jnp.maximum(peak, jnp.max(jnp.abs(centroids)).astype(F32))[None]
    unit = finish(acc, 1.0 / peak, centroids, where)[None]

    shifts = [0, 1, nz - 1] + list(range(2, nz - 1))
    held = [unit] + [
        lax.ppermute(unit, "z", [(i, (i + s) % nz) for i in range(nz)]) for s in shifts[1:]
    ]
    held = jnp.concatenate(held, axis=0)
    from_x = lax.ppermute(held, "x", SWAP)
    from_y = lax.ppermute(held, "y", SWAP)
    cut = nz // 2
    diagonal = jnp.concatenate(
        [lax.ppermute(from_y[:cut], "x", SWAP), lax.ppermute(from_x[cut:], "y", SWAP)], axis=0
    )
    sources = (z - jnp.array(shifts, I32)) % nz * ny
    out = spread(held, from_x, sources + y, x[None], peak, width, None)
    out = spread(from_y, diagonal, sources + (1 - y), x[None], peak, width, out)

    point_f = points.astype(F32)
    point_sq = jnp.sum(point_f * point_f, axis=1)
    best = jnp.minimum(nearest(points, point_sq, centroids), nearest(points, point_sq, others))
    return out, best / width


def split_dp(mesh, width):
    dp, mp = mesh.shape["dp"], mesh.shape["mp"]
    owners = width // COLS
    devices = mesh.devices.reshape(dp // owners, owners // 4, 2, 2, mp)
    return Mesh(devices, AXES)


def solution(mesh):
    rows = P(AXES)

    def step(points, centroids, assign, keep_mask):
        return jax.shard_map(
            shards,
            mesh=split_dp(mesh, points.shape[1]),
            in_specs=(P(AXES, None), P("mp", None), rows, rows),
            out_specs=(P("mp", None), rows),
            check_vma=False,
        )(points, centroids, assign, keep_mask)

    return step
```

```python
import functools

import jax
import jax.numpy as jnp
from jax import lax
from jax.experimental import pallas as pl
from jax.experimental.pallas import tpu as pltpu
from jax.sharding import Mesh, PartitionSpec as P


LANES = 128
COLS = 64
LOW = 4
DIGIT = 7
CODE_ROWS = 16
LEVELS = 32767.0
TINY = 1e-30
GROUP = 8
SMALL_VMEM = 24 << 20
F32, BF16, I32 = jnp.float32, jnp.bfloat16, jnp.int32
HALF = LANES // 2
SWAP = [(0, 1), (1, 0)]
OWNERS = ("z", "y", "x")
AXES = ("g",) + OWNERS + ("mp",)

VMEM = pl.BlockSpec(memory_space=pltpu.VMEM)
SMEM = pl.BlockSpec(memory_space=pltpu.SMEM)


def pack_kernel(points_ref, assign_ref, keep_ref, out_ref):
    rows, width = points_ref.shape
    blocks = rows // LANES
    kept = keep_ref[...]
    assign = assign_ref[...]
    high = jnp.where(kept > 0, assign >> DIGIT, -1).astype(F32)
    low = (assign & ((1 << DIGIT) - 1)).astype(F32)
    weight = kept.astype(F32)
    peak = jnp.zeros((1, LANES), F32)
    for b in range(blocks):
        for c in range(width // LANES):
            tile = points_ref[b * LANES : (b + 1) * LANES, c * LANES : (c + 1) * LANES].T
            out_ref[2 * c, b * COLS : (b + 1) * COLS, :] = tile[:COLS]
            out_ref[2 * c + 1, b * COLS : (b + 1) * COLS, :] = tile[COLS:]
            size = jnp.max(jnp.abs(tile.astype(F32)), axis=0, keepdims=True)
            peak = jnp.maximum(peak, size * weight[b : b + 1])
    pad = jnp.zeros((CODE_ROWS - 2 * blocks - 1, LANES), F32)
    codes = jnp.concatenate([high, low, peak, pad], axis=0).astype(BF16)
    for s in range(out_ref.shape[0]):
        out_ref[s, blocks * COLS :, :] = codes


def pack(points, assign, keep):
    rows, width = points.shape
    blocks = rows // LANES
    assert 2 * blocks + 1 <= CODE_ROWS
    shape = (width // COLS, blocks * COLS + CODE_ROWS, LANES)
    return pl.pallas_call(
        pack_kernel,
        out_shape=jax.ShapeDtypeStruct(shape, BF16),
        in_specs=[VMEM] * 3,
        out_specs=VMEM,
        cost_estimate=pl.CostEstimate(
            flops=2 * rows * width, bytes_accessed=4 * rows * width, transcendentals=0
        ),
        name="pack",
    )(points, assign.reshape(blocks, LANES), keep.reshape(blocks, LANES))


def add_sources(base, recv_ref, acc_ref):
    sources, height, _ = recv_ref.shape
    high_size = acc_ref.shape[1]
    blocks = (height - CODE_ROWS) // COLS
    rows = blocks * LANES
    shift = high_size.bit_length() - 1

    group = min(GROUP, sources)

    def factors(s):
        codes = recv_ref[s, blocks * COLS :, :].astype(F32)
        local = (codes[:blocks] * float(1 << DIGIT) + codes[blocks : 2 * blocks]).astype(I32) - base
        local = jnp.concatenate([local[b : b + 1] for b in range(blocks)], axis=1)
        k_low, k_high = local >> shift, local & (high_size - 1)
        hot = (lax.broadcasted_iota(I32, (high_size, rows), 0) == k_high).astype(F32).astype(BF16)
        data = [recv_ref[s, b * COLS : (b + 1) * COLS, :] for b in range(blocks)]
        data = jnp.concatenate(data, axis=1)
        masks = [(k_low == l).astype(F32) for l in range(LOW)]
        parts = [data * m.astype(BF16) for m in masks]
        pad = jnp.zeros((CODE_ROWS - LOW, rows), F32)
        parts.append(jnp.concatenate(masks + [pad], axis=0).astype(BF16))
        return jnp.concatenate(parts, axis=0), hot, codes[2 * blocks : 2 * blocks + 1]

    def step(i, peak):
        left, hot, size = zip(*[factors(i * group + u) for u in range(group)])
        left, hot = jnp.concatenate(left, axis=1), jnp.concatenate(hot, axis=1)
        acc_ref[...] += lax.dot_general(
            left, hot, (((1,), (1,)), ((), ())), preferred_element_type=F32
        )
        return functools.reduce(jnp.maximum, size, peak)

    return lax.fori_loop(0, sources // group, step, jnp.zeros((1, LANES), F32))


def finish(where_ref, acc_ref, scale, prior_ref, out_ref):
    high_size = acc_ref.shape[1]
    counts = acc_ref[LOW * COLS : LOW * COLS + 8, :]
    inverse = 1.0 / jnp.maximum(counts, 1.0)
    tall = counts.T
    odd = where_ref[1] > 0
    lower = lax.broadcasted_iota(I32, (high_size, LANES), 1) < HALF
    for l in range(0, LOW, 2):
        mean = [acc_ref[k * COLS : (k + 1) * COLS, :] * inverse[k : k + 1] for k in (l, l + 1)]
        mean = jnp.concatenate(mean, axis=0).T
        priors = [prior_ref[k * high_size : (k + 1) * high_size, :].astype(F32) for k in (l, l + 1)]
        turned = [pltpu.roll(p, HALF, 1) for p in priors]
        prior = jnp.where(
            lower, jnp.where(odd, turned[0], priors[0]), jnp.where(odd, priors[1], turned[1])
        )
        count = jnp.where(lower, tall[:, l : l + 1], tall[:, l + 1 : l + 2])
        value = jnp.where(count > 0.5, mean, prior)
        root = jnp.sqrt(jnp.sqrt(jnp.abs(value) * scale))
        level = jnp.minimum(root * LEVELS + 0.5, LEVELS).astype(I32)
        level = jnp.where(value < 0, -level, level).astype(jnp.int16)
        out_ref[:, l * COLS : (l + 2) * COLS] = level


def first_kernel(where_ref, recv_ref, acc_ref, peak_ref):
    acc_ref[...] = jnp.zeros_like(acc_ref)
    peak = add_sources(where_ref[0], recv_ref, acc_ref)
    peak_ref[...] = jnp.broadcast_to(peak, peak_ref.shape)


def second_kernel(where_ref, recv_ref, given_ref, given_peak_ref, acc_ref, peak_ref):
    acc_ref[...] = given_ref[...]
    peak = add_sources(where_ref[0], recv_ref, acc_ref)
    peak_ref[...] = jnp.maximum(given_peak_ref[...], peak)


def last_kernel(where_ref, least_ref, recv_ref, given_ref, given_peak_ref, prior_ref, out_ref, peak_ref, acc_ref):
    acc_ref[...] = given_ref[...]
    peak = jnp.maximum(given_peak_ref[...], add_sources(where_ref[0], recv_ref, acc_ref))
    peak = jnp.maximum(jnp.max(peak), least_ref[0])
    peak_ref[0] = peak
    finish(where_ref, acc_ref, 1.0 / peak, prior_ref, out_ref)


def finish_kernel(where_ref, peak_ref, acc_ref, prior_ref, out_ref):
    finish(where_ref, acc_ref, 1.0 / peak_ref[0], prior_ref, out_ref)


def sums_cost(recv, high_size):
    sources, height, _ = recv.shape
    rows = (height - CODE_ROWS) // COLS * LANES * sources
    flops = 2 * rows * (LOW * COLS + CODE_ROWS) * high_size
    return pl.CostEstimate(flops=flops, bytes_accessed=recv.size * 2, transcendentals=0)


def sums_of(recv, where, given, high_size):
    shapes = (
        jax.ShapeDtypeStruct((LOW * COLS + CODE_ROWS, high_size), F32),
        jax.ShapeDtypeStruct((8, LANES), F32),
    )
    return pl.pallas_call(
        first_kernel if given is None else second_kernel,
        out_shape=shapes,
        in_specs=[SMEM, VMEM] + ([] if given is None else [VMEM, VMEM]),
        out_specs=(VMEM, VMEM),
        cost_estimate=sums_cost(recv, high_size),
        compiler_params=pltpu.CompilerParams(vmem_limit_bytes=SMALL_VMEM),
        name="sums_first" if given is None else "sums_second",
    )(where, recv, *(given or ()))


def unit_shape(high_size):
    return jax.ShapeDtypeStruct((high_size, LOW * COLS), jnp.int16)


def last_sums(recv, where, given, least, prior, high_size):
    return pl.pallas_call(
        last_kernel,
        out_shape=(unit_shape(high_size), jax.ShapeDtypeStruct((1,), F32)),
        in_specs=[SMEM, SMEM, VMEM, VMEM, VMEM, VMEM],
        out_specs=(VMEM, SMEM),
        scratch_shapes=[pltpu.VMEM(given[0].shape, F32)],
        cost_estimate=sums_cost(recv, high_size),
        compiler_params=pltpu.CompilerParams(vmem_limit_bytes=SMALL_VMEM),
        name="sums_last",
    )(where, least, recv, *given, prior)


def finished(acc, peak, prior, where):
    return pl.pallas_call(
        finish_kernel,
        out_shape=unit_shape(acc.shape[1]),
        in_specs=[SMEM, SMEM, VMEM, VMEM],
        out_specs=VMEM,
        name="finish",
    )(where, peak, acc, prior)


def spread_kernel(parts, where_ref, peak_ref, own_ref, x_piece_ref, y_piece_ref, *refs):
    out_ref = refs[-1]
    high_size = own_ref.shape[0]
    first = where_ref[1] == 0
    y = where_ref[2]

    def emit(mine_ref, at, other_ref, column):
        rows = other_ref.shape[0]
        lower = lax.broadcasted_iota(jnp.int16, (rows, LANES), 1) < HALF
        lanes = pl.ds(pl.multiple_of(column * LANES, LANES), LANES)
        mine, other = mine_ref[at : at + rows, :], other_ref[...]
        left, right = jnp.where(first, mine, other), jnp.where(first, other, mine)
        both = (
            jnp.where(lower, left, pltpu.roll(right, HALF, 1)),
            jnp.where(lower, pltpu.roll(left, HALF, 1), right),
        )
        for k, level in enumerate(both):
            t = level.astype(I32).astype(F32) * (1.0 / LEVELS)
            s = t * jnp.abs(t)
            start = k * high_size + at
            out_ref[start : start + rows, lanes] = s * jnp.abs(s) * peak_ref[0]

    emit(own_ref, 0, x_piece_ref, y)
    at = 0
    for ref in refs[:parts]:
        emit(y_piece_ref, at, ref, 1 - y)
        at += ref.shape[0]


def spread(n, own, x_piece, y_piece, diagonal, where, peak, width, into):
    high_size, _ = own.shape
    total = LOW * high_size
    pieces = [own, x_piece, y_piece, *diagonal]
    extra = [] if into is None else [into]
    return pl.pallas_call(
        functools.partial(spread_kernel, len(diagonal)),
        grid_spec=pltpu.PrefetchScalarGridSpec(
            num_scalar_prefetch=1,
            grid=(LOW // 2,),
            in_specs=[SMEM]
            + [pl.BlockSpec((p.shape[0], LANES), lambda i, w: (0, i)) for p in pieces]
            + [pl.BlockSpec(memory_space=pl.ANY) for _ in extra],
            out_specs=pl.BlockSpec((2 * high_size, 2 * LANES), lambda i, w: (i, w[3 + n])),
        ),
        out_shape=jax.ShapeDtypeStruct((total, width), F32),
        input_output_aliases={2 + len(pieces): 0} if extra else {},
        cost_estimate=pl.CostEstimate(
            flops=16 * total * LANES, bytes_accessed=12 * total * LANES, transcendentals=0
        ),
        compiler_params=pltpu.CompilerParams(vmem_limit_bytes=SMALL_VMEM),
        name="spread",
    )(where, peak, *pieces, *extra)


def z_shifts(nz):
    return [0, 1, nz - 1] + list(range(2, nz - 1))


def gather(unit, peak, where, width):
    nz = lax.axis_size("z")
    rows = unit.shape[0]
    held = [unit]
    for n, s in enumerate(z_shifts(nz)[1:], 1):
        held.append(lax.ppermute(unit, "z", [(i, (i + s) % nz) for i in range(nz)]))
    out = None
    for n, piece in enumerate(held):
        from_x = lax.ppermute(piece, "x", SWAP)
        from_y = lax.ppermute(piece, "y", SWAP)
        cut = (rows, 0)[n] if n < 2 else rows // 2
        diagonal = []
        if cut:
            diagonal.append(lax.ppermute(from_y[:cut], "x", SWAP))
        if cut < rows:
            diagonal.append(lax.ppermute(from_x[cut:], "y", SWAP))
        out = spread(n, piece, from_x, from_y, diagonal, where, peak, width, out)
    return out


def nearest(points, point_sq, part):
    inner = lax.dot_general(points, part, (((1,), (1,)), ((), ())), preferred_element_type=F32)
    part_f = part.astype(F32)
    part_sq = jnp.sum(part_f * part_f, axis=1)
    return jnp.min(point_sq[:, None] - 2.0 * inner + part_sq[None, :], axis=1)


def shards(points, centroids, assign, keep_mask):
    width = points.shape[1]
    shard_rows = centroids.shape[0]
    high_size = shard_rows // LOW
    z, y, x = (lax.axis_index(a) for a in OWNERS)
    nz, ny, nx = (lax.axis_size(a) for a in OWNERS)
    assert nx == 2 and ny == 2 and nz * ny * nx * COLS == width
    block = z * ny + y
    blocks = [(z - s) % nz for s in z_shifts(nz)]
    where = jnp.stack([lax.axis_index("mp") * shard_rows, x, y, *blocks]).astype(I32)

    parcels = pack(points, assign, keep_mask)
    recv = lax.all_to_all(parcels, OWNERS, 0, 0, tiled=True)
    others = lax.ppermute(centroids, "mp", SWAP)

    point_f = points.astype(F32)
    point_sq = jnp.sum(point_f * point_f, axis=1)
    best = jnp.minimum(nearest(points, point_sq, centroids), nearest(points, point_sq, others))
    least = jnp.maximum(jnp.max(jnp.abs(centroids)).astype(F32), TINY)[None]
    prior = lax.dynamic_slice_in_dim(centroids, block * LANES, LANES, 1)
    recv, best, least, prior, where = lax.optimization_barrier((recv, best, least, prior, where))

    partner = lax.ppermute(recv, "mp", SWAP)
    given = sums_of(recv, where, None, high_size)
    if lax.axis_size("g") > 1:
        acc, peak = sums_of(partner, where, given, high_size)
        acc, peak = lax.psum(acc, "g"), lax.pmax(jnp.max(peak), "g")
        peak = jnp.maximum(peak, least)
        unit = finished(acc, peak, prior, where)
    else:
        unit, peak = last_sums(partner, where, given, least, prior, high_size)

    out = gather(unit, peak, where, width)
    return out, best / width


def split_dp(mesh, width):
    dp, mp = mesh.shape["dp"], mesh.shape["mp"]
    owners = width // COLS
    devices = mesh.devices.reshape(dp // owners, owners // 4, 2, 2, mp)
    return Mesh(devices, AXES)


def solution(mesh):
    rows = P(AXES)

    def step(points, centroids, assign, keep_mask):
        return jax.shard_map(
            shards,
            mesh=split_dp(mesh, points.shape[1]),
            in_specs=(P(AXES, None), P("mp", None), rows, rows),
            out_specs=(P("mp", None), rows),
            check_vma=False,
        )(points, centroids, assign, keep_mask)

    return step
```

```python
import functools

import jax
import jax.numpy as jnp
from jax import lax
from jax.experimental import pallas as pl
from jax.experimental.pallas import tpu as pltpu
from jax.sharding import Mesh, PartitionSpec as P


LANES = 128
COLS = 64
LOW = 4
DIGIT = 7
CODE_ROWS = 16
LEVELS = 32767.0
TINY = 1e-30
GROUP = 8
SMALL_VMEM = 24 << 20
F32, BF16, I32 = jnp.float32, jnp.bfloat16, jnp.int32
HALF = LANES // 2
SWAP = [(0, 1), (1, 0)]
OWNERS = ("z", "y", "x")
AXES = ("g",) + OWNERS + ("mp",)

SPREADS = ((0, 2), (2, 5), (5, 8))
VMEM = pl.BlockSpec(memory_space=pltpu.VMEM)
SMEM = pl.BlockSpec(memory_space=pltpu.SMEM)


def pack_kernel(points_ref, assign_ref, keep_ref, out_ref):
    rows, width = points_ref.shape
    blocks = rows // LANES
    kept = keep_ref[...]
    assign = assign_ref[...]
    high = jnp.where(kept > 0, assign >> DIGIT, -1).astype(F32)
    low = (assign & ((1 << DIGIT) - 1)).astype(F32)
    weight = kept.astype(F32)
    peak = jnp.zeros((1, LANES), F32)
    for b in range(blocks):
        for c in range(width // LANES):
            tile = points_ref[b * LANES : (b + 1) * LANES, c * LANES : (c + 1) * LANES].T
            out_ref[2 * c, b * COLS : (b + 1) * COLS, :] = tile[:COLS]
            out_ref[2 * c + 1, b * COLS : (b + 1) * COLS, :] = tile[COLS:]
            size = jnp.max(jnp.abs(tile.astype(F32)), axis=0, keepdims=True)
            peak = jnp.maximum(peak, size * weight[b : b + 1])
    pad = jnp.zeros((CODE_ROWS - 2 * blocks - 1, LANES), F32)
    codes = jnp.concatenate([high, low, peak, pad], axis=0).astype(BF16)
    for s in range(out_ref.shape[0]):
        out_ref[s, blocks * COLS :, :] = codes


def pack(points, assign, keep):
    rows, width = points.shape
    blocks = rows // LANES
    assert 2 * blocks + 1 <= CODE_ROWS
    shape = (width // COLS, blocks * COLS + CODE_ROWS, LANES)
    return pl.pallas_call(
        pack_kernel,
        out_shape=jax.ShapeDtypeStruct(shape, BF16),
        in_specs=[VMEM] * 3,
        out_specs=VMEM,
        cost_estimate=pl.CostEstimate(
            flops=2 * rows * width, bytes_accessed=4 * rows * width, transcendentals=0
        ),
        name="pack",
    )(points, assign.reshape(blocks, LANES), keep.reshape(blocks, LANES))


def add_sources(base, recv_ref, acc_ref):
    sources, height, _ = recv_ref.shape
    high_size = acc_ref.shape[1]
    blocks = (height - CODE_ROWS) // COLS
    rows = blocks * LANES
    shift = high_size.bit_length() - 1

    group = min(GROUP, sources)

    def factors(s):
        codes = recv_ref[s, blocks * COLS :, :].astype(F32)
        local = (codes[:blocks] * float(1 << DIGIT) + codes[blocks : 2 * blocks]).astype(I32) - base
        local = jnp.concatenate([local[b : b + 1] for b in range(blocks)], axis=1)
        k_low, k_high = local >> shift, local & (high_size - 1)
        hot = (lax.broadcasted_iota(I32, (high_size, rows), 0) == k_high).astype(F32).astype(BF16)
        data = [recv_ref[s, b * COLS : (b + 1) * COLS, :] for b in range(blocks)]
        data = jnp.concatenate(data, axis=1)
        masks = [(k_low == l).astype(F32) for l in range(LOW)]
        parts = [data * m.astype(BF16) for m in masks]
        pad = jnp.zeros((CODE_ROWS - LOW, rows), F32)
        parts.append(jnp.concatenate(masks + [pad], axis=0).astype(BF16))
        return jnp.concatenate(parts, axis=0), hot, codes[2 * blocks : 2 * blocks + 1]

    def step(i, peak):
        left, hot, size = zip(*[factors(i * group + u) for u in range(group)])
        left, hot = jnp.concatenate(left, axis=1), jnp.concatenate(hot, axis=1)
        acc_ref[...] += lax.dot_general(
            left, hot, (((1,), (1,)), ((), ())), preferred_element_type=F32
        )
        return functools.reduce(jnp.maximum, size, peak)

    return lax.fori_loop(0, sources // group, step, jnp.zeros((1, LANES), F32))


def finish(where_ref, acc_ref, scale, prior_ref, out_ref):
    high_size = acc_ref.shape[1]
    counts = acc_ref[LOW * COLS : LOW * COLS + 8, :]
    inverse = 1.0 / jnp.maximum(counts, 1.0)
    tall = counts.T
    odd = where_ref[1] > 0
    lower = lax.broadcasted_iota(I32, (high_size, LANES), 1) < HALF
    for l in range(0, LOW, 2):
        mean = [acc_ref[k * COLS : (k + 1) * COLS, :] * inverse[k : k + 1] for k in (l, l + 1)]
        mean = jnp.concatenate(mean, axis=0).T
        priors = [prior_ref[k * high_size : (k + 1) * high_size, :].astype(F32) for k in (l, l + 1)]
        turned = [pltpu.roll(p, HALF, 1) for p in priors]
        prior = jnp.where(
            lower, jnp.where(odd, turned[0], priors[0]), jnp.where(odd, priors[1], turned[1])
        )
        count = jnp.where(lower, tall[:, l : l + 1], tall[:, l + 1 : l + 2])
        value = jnp.where(count > 0.5, mean, prior)
        root = jnp.sqrt(jnp.sqrt(jnp.abs(value) * scale))
        level = jnp.minimum(root * LEVELS + 0.5, LEVELS).astype(I32)
        level = jnp.where(value < 0, -level, level).astype(jnp.int16)
        out_ref[:, l * COLS : (l + 2) * COLS] = level


def first_kernel(where_ref, recv_ref, acc_ref, peak_ref):
    acc_ref[...] = jnp.zeros_like(acc_ref)
    peak = add_sources(where_ref[0], recv_ref, acc_ref)
    peak_ref[...] = jnp.broadcast_to(peak, peak_ref.shape)


def second_kernel(where_ref, recv_ref, given_ref, given_peak_ref, acc_ref, peak_ref):
    acc_ref[...] = given_ref[...]
    peak = add_sources(where_ref[0], recv_ref, acc_ref)
    peak_ref[...] = jnp.maximum(given_peak_ref[...], peak)


def last_kernel(where_ref, least_ref, recv_ref, given_ref, given_peak_ref, prior_ref, out_ref, peak_ref, acc_ref):
    acc_ref[...] = given_ref[...]
    peak = jnp.maximum(given_peak_ref[...], add_sources(where_ref[0], recv_ref, acc_ref))
    peak = jnp.maximum(jnp.max(peak), least_ref[0])
    peak_ref[0] = peak
    finish(where_ref, acc_ref, 1.0 / peak, prior_ref, out_ref)


def finish_kernel(where_ref, peak_ref, acc_ref, prior_ref, out_ref):
    finish(where_ref, acc_ref, 1.0 / peak_ref[0], prior_ref, out_ref)


def sums_cost(recv, high_size):
    sources, height, _ = recv.shape
    rows = (height - CODE_ROWS) // COLS * LANES * sources
    flops = 2 * rows * (LOW * COLS + CODE_ROWS) * high_size
    return pl.CostEstimate(flops=flops, bytes_accessed=recv.size * 2, transcendentals=0)


def sums_of(recv, where, given, high_size):
    shapes = (
        jax.ShapeDtypeStruct((LOW * COLS + CODE_ROWS, high_size), F32),
        jax.ShapeDtypeStruct((8, LANES), F32),
    )
    return pl.pallas_call(
        first_kernel if given is None else second_kernel,
        out_shape=shapes,
        in_specs=[SMEM, VMEM] + ([] if given is None else [VMEM, VMEM]),
        out_specs=(VMEM, VMEM),
        cost_estimate=sums_cost(recv, high_size),
        compiler_params=pltpu.CompilerParams(vmem_limit_bytes=SMALL_VMEM),
        name="sums_first" if given is None else "sums_second",
    )(where, recv, *(given or ()))


def unit_shape(high_size):
    return jax.ShapeDtypeStruct((high_size, LOW * COLS), jnp.int16)


def last_sums(recv, where, given, least, prior, high_size):
    return pl.pallas_call(
        last_kernel,
        out_shape=(unit_shape(high_size), jax.ShapeDtypeStruct((1,), F32)),
        in_specs=[SMEM, SMEM, VMEM, VMEM, VMEM, VMEM],
        out_specs=(VMEM, SMEM),
        scratch_shapes=[pltpu.VMEM(given[0].shape, F32)],
        cost_estimate=sums_cost(recv, high_size),
        compiler_params=pltpu.CompilerParams(vmem_limit_bytes=SMALL_VMEM),
        name="sums_last",
    )(where, least, recv, *given, prior)


def finished(acc, peak, prior, where):
    return pl.pallas_call(
        finish_kernel,
        out_shape=unit_shape(acc.shape[1]),
        in_specs=[SMEM, SMEM, VMEM, VMEM],
        out_specs=VMEM,
        name="finish",
    )(where, peak, acc, prior)


def spread_kernel(counts, where_ref, peak_ref, *refs):
    out_ref = refs[-1]
    first = where_ref[1] == 0
    high_size = out_ref.shape[0] // LOW

    def emit(mine_ref, other_refs):
        at = 0
        for other_ref in other_refs:
            rows = other_ref.shape[0]
            lower = lax.broadcasted_iota(jnp.int16, (rows, LANES), 1) < HALF
            for l in range(0, LOW, 2):
                lanes = slice(l * COLS, (l + 2) * COLS)
                mine, other = mine_ref[at : at + rows, lanes], other_ref[:, lanes]
                left, right = jnp.where(first, mine, other), jnp.where(first, other, mine)
                both = (
                    jnp.where(lower, left, pltpu.roll(right, HALF, 1)),
                    jnp.where(lower, pltpu.roll(left, HALF, 1), right),
                )
                for k, level in enumerate(both):
                    t = level.astype(I32).astype(F32) * (1.0 / LEVELS)
                    s = t * jnp.abs(t)
                    start = (l + k) * high_size + at
                    out_ref[start : start + rows, :] = s * jnp.abs(s) * peak_ref[0]
            at += rows

    at = 0
    for p, count in enumerate(counts):
        pl.when(pl.program_id(0) == p)(functools.partial(emit, refs[at], refs[at + 1 : at + 1 + count]))
        at += 1 + count


def spread(first, pairs, where, peak, width, into):
    high_size = pairs[0][0].shape[0]
    total = LOW * high_size
    pieces = [p for mine, others in pairs for p in (mine, *others)]
    extra = [] if into is None else [into]
    return pl.pallas_call(
        functools.partial(spread_kernel, tuple(len(others) for _, others in pairs)),
        grid_spec=pltpu.PrefetchScalarGridSpec(
            num_scalar_prefetch=1,
            grid=(len(pairs),),
            in_specs=[SMEM] + [VMEM for _ in pieces] + [pl.BlockSpec(memory_space=pl.ANY) for _ in extra],
            out_specs=pl.BlockSpec((total, LANES), lambda p, w: (0, w[2 + first + p])),
        ),
        out_shape=jax.ShapeDtypeStruct((total, width), F32),
        input_output_aliases={2 + len(pieces): 0} if extra else {},
        cost_estimate=pl.CostEstimate(
            flops=8 * len(pairs) * total * LANES,
            bytes_accessed=6 * len(pairs) * total * LANES,
            transcendentals=0,
        ),
        compiler_params=pltpu.CompilerParams(vmem_limit_bytes=SMALL_VMEM),
        name="spread",
    )(where, peak, *pieces, *extra)


def z_shifts(nz):
    return [0, 1, nz - 1] + list(range(2, nz - 1))


def gather(unit, peak, where, width):
    nz = lax.axis_size("z")
    assert nz == 4
    half = unit.shape[0] // 2

    def send(piece, axis, shift=1):
        size = lax.axis_size(axis)
        return lax.ppermute(piece, axis, [(i, (i + shift) % size) for i in range(size)])

    shifts = z_shifts(nz)
    held = [unit] + [send(unit, "z", shifts[n]) for n in range(1, nz)]
    from_x = [send(piece, "x") for piece in held]
    from_y = [send(piece, "y") for piece in held]
    near = send(from_y[0], "x")
    diagonal = [
        [near],
        [send(from_x[1], "y")],
        [send(from_y[2][:half], "x"), send(from_x[2][half:], "y")],
        [send(near, "z", shifts[3])],
    ]
    pairs = []
    for n in range(nz):
        pairs += [(held[n], [from_x[n]]), (from_y[n], diagonal[n])]
    out = None
    for start, end in SPREADS:
        out = spread(start, pairs[start:end], where, peak, width, out)
    return out


def nearest(points, point_sq, part):
    inner = lax.dot_general(points, part, (((1,), (1,)), ((), ())), preferred_element_type=F32)
    part_f = part.astype(F32)
    part_sq = jnp.sum(part_f * part_f, axis=1)
    return jnp.min(point_sq[:, None] - 2.0 * inner + part_sq[None, :], axis=1)


def shards(points, centroids, assign, keep_mask):
    width = points.shape[1]
    shard_rows = centroids.shape[0]
    high_size = shard_rows // LOW
    z, y, x = (lax.axis_index(a) for a in OWNERS)
    nz, ny, nx = (lax.axis_size(a) for a in OWNERS)
    assert nx == 2 and ny == 2 and nz * ny * nx * COLS == width
    block = z * ny + y
    columns = [((z - s) % nz) * ny + (y ^ m) for s in z_shifts(nz) for m in range(ny)]
    where = jnp.stack([lax.axis_index("mp") * shard_rows, x, *columns]).astype(I32)

    parcels = pack(points, assign, keep_mask)
    recv = lax.all_to_all(parcels, OWNERS, 0, 0, tiled=True)
    others = lax.ppermute(centroids, "mp", SWAP)

    point_f = points.astype(F32)
    point_sq = jnp.sum(point_f * point_f, axis=1)
    best = jnp.minimum(nearest(points, point_sq, centroids), nearest(points, point_sq, others))
    least = jnp.maximum(jnp.max(jnp.abs(centroids)).astype(F32), TINY)[None]
    prior = lax.dynamic_slice_in_dim(centroids, block * LANES, LANES, 1)
    recv, best, least, prior, where = lax.optimization_barrier((recv, best, least, prior, where))

    partner = lax.ppermute(recv, "mp", SWAP)
    given = sums_of(recv, where, None, high_size)
    if lax.axis_size("g") > 1:
        acc, peak = sums_of(partner, where, given, high_size)
        acc, peak = lax.psum(acc, "g"), lax.pmax(jnp.max(peak), "g")
        peak = jnp.maximum(peak, least)
        unit = finished(acc, peak, prior, where)
    else:
        unit, peak = last_sums(partner, where, given, least, prior, high_size)

    out = gather(unit, peak, where, width)
    return out, best / width


def split_dp(mesh, width):
    dp, mp = mesh.shape["dp"], mesh.shape["mp"]
    owners = width // COLS
    devices = mesh.devices.reshape(dp // owners, owners // 4, 2, 2, mp)
    return Mesh(devices, AXES)


def solution(mesh):
    rows = P(AXES)

    def step(points, centroids, assign, keep_mask):
        return jax.shard_map(
            shards,
            mesh=split_dp(mesh, points.shape[1]),
            in_specs=(P(AXES, None), P("mp", None), rows, rows),
            out_specs=(P("mp", None), rows),
            check_vma=False,
        )(points, centroids, assign, keep_mask)

    return step
```

```python
import functools

import jax
import jax.numpy as jnp
from jax import lax
from jax.experimental import pallas as pl
from jax.experimental.pallas import tpu as pltpu
from jax.sharding import Mesh, PartitionSpec as P


LANES = 128
COLS = 64
LOW = 4
DIGIT = 7
CODE_ROWS = 16
LEVELS = 32767.0
TINY = 1e-30
GROUP = 16
SMALL_VMEM = 24 << 20
F32, BF16, I32 = jnp.float32, jnp.bfloat16, jnp.int32
HALF = LANES // 2
SWAP = [(0, 1), (1, 0)]
OWNERS = ("z", "y", "x")
AXES = ("g",) + OWNERS + ("mp",)

PAIRS = ((0, 0), (0, 1), (1, 0), (2, 0), (1, 1), (3, 0), (3, 1), (2, 1))
SPREADS = ((0, 2), (2, 4), (4, 6), (6, 8))
VMEM = pl.BlockSpec(memory_space=pltpu.VMEM)
SMEM = pl.BlockSpec(memory_space=pltpu.SMEM)


def pack_kernel(far_ref, assign_ref, keep_ref, out_ref, points_ref, sems):
    rows, width = points_ref.shape
    blocks = rows // LANES
    copies = []
    for b in range(blocks):
        part = pl.ds(b * LANES, LANES)
        copies.append(pltpu.make_async_copy(far_ref.at[part], points_ref.at[part], sems.at[b]))
        copies[b].start()
    kept = keep_ref[...]
    assign = assign_ref[...]
    high = jnp.where(kept > 0, assign >> DIGIT, -1).astype(F32)
    low = (assign & ((1 << DIGIT) - 1)).astype(F32)
    weight = kept.astype(F32)
    peak = jnp.zeros((1, LANES), F32)
    for b in range(blocks):
        copies[b].wait()
        for c in range(width // LANES):
            tile = points_ref[b * LANES : (b + 1) * LANES, c * LANES : (c + 1) * LANES].T
            out_ref[2 * c, b * COLS : (b + 1) * COLS, :] = tile[:COLS]
            out_ref[2 * c + 1, b * COLS : (b + 1) * COLS, :] = tile[COLS:]
            size = jnp.max(jnp.abs(tile.astype(F32)), axis=0, keepdims=True)
            peak = jnp.maximum(peak, size * weight[b : b + 1])
    pad = jnp.zeros((CODE_ROWS - 2 * blocks - 1, LANES), F32)
    codes = jnp.concatenate([high, low, peak, pad], axis=0).astype(BF16)
    for s in range(out_ref.shape[0]):
        out_ref[s, blocks * COLS :, :] = codes


def pack(points, assign, keep):
    rows, width = points.shape
    blocks = rows // LANES
    assert 2 * blocks + 1 <= CODE_ROWS
    shape = (width // COLS, blocks * COLS + CODE_ROWS, LANES)
    return pl.pallas_call(
        pack_kernel,
        out_shape=jax.ShapeDtypeStruct(shape, BF16),
        in_specs=[pl.BlockSpec(memory_space=pl.ANY), VMEM, VMEM],
        out_specs=VMEM,
        scratch_shapes=[pltpu.VMEM((rows, width), BF16), pltpu.SemaphoreType.DMA((blocks,))],
        cost_estimate=pl.CostEstimate(
            flops=2 * rows * width, bytes_accessed=4 * rows * width, transcendentals=0
        ),
        name="pack",
    )(points, assign.reshape(blocks, LANES), keep.reshape(blocks, LANES))


def add_sources(base, recv_ref, acc_ref):
    sources, height, _ = recv_ref.shape
    high_size = acc_ref.shape[1]
    blocks = (height - CODE_ROWS) // COLS
    rows = blocks * LANES
    shift = high_size.bit_length() - 1

    group = min(GROUP, sources)

    def factors(s):
        codes = recv_ref[s, blocks * COLS :, :].astype(F32)
        local = (codes[:blocks] * float(1 << DIGIT) + codes[blocks : 2 * blocks]).astype(I32) - base
        local = jnp.concatenate([local[b : b + 1] for b in range(blocks)], axis=1)
        k_low, k_high = local >> shift, local & (high_size - 1)
        hot = (lax.broadcasted_iota(I32, (high_size, rows), 0) == k_high).astype(F32).astype(BF16)
        data = [recv_ref[s, b * COLS : (b + 1) * COLS, :] for b in range(blocks)]
        data = jnp.concatenate(data, axis=1)
        masks = [(k_low == l).astype(F32) for l in range(LOW)]
        parts = [data * m.astype(BF16) for m in masks]
        pad = jnp.zeros((CODE_ROWS - LOW, rows), F32)
        parts.append(jnp.concatenate(masks + [pad], axis=0).astype(BF16))
        return jnp.concatenate(parts, axis=0), hot, codes[2 * blocks : 2 * blocks + 1]

    def step(i, peak):
        left, hot, size = zip(*[factors(i * group + u) for u in range(group)])
        left, hot = jnp.concatenate(left, axis=1), jnp.concatenate(hot, axis=1)
        acc_ref[...] += lax.dot_general(
            left, hot, (((1,), (1,)), ((), ())), preferred_element_type=F32
        )
        return functools.reduce(jnp.maximum, size, peak)

    return lax.fori_loop(0, sources // group, step, jnp.zeros((1, LANES), F32))


def finish(where_ref, acc_ref, scale, prior_ref, out_ref):
    high_size = acc_ref.shape[1]
    counts = acc_ref[LOW * COLS : LOW * COLS + 8, :]
    inverse = 1.0 / jnp.maximum(counts, 1.0)
    tall = counts.T
    odd = where_ref[1] > 0
    lower = lax.broadcasted_iota(I32, (high_size, LANES), 1) < HALF
    for l in range(0, LOW, 2):
        mean = [acc_ref[k * COLS : (k + 1) * COLS, :] * inverse[k : k + 1] for k in (l, l + 1)]
        mean = jnp.concatenate(mean, axis=0).T
        priors = [prior_ref[k * high_size : (k + 1) * high_size, :].astype(F32) for k in (l, l + 1)]
        turned = [pltpu.roll(p, HALF, 1) for p in priors]
        prior = jnp.where(
            lower, jnp.where(odd, turned[0], priors[0]), jnp.where(odd, priors[1], turned[1])
        )
        count = jnp.where(lower, tall[:, l : l + 1], tall[:, l + 1 : l + 2])
        value = jnp.where(count > 0.5, mean, prior)
        root = jnp.sqrt(jnp.sqrt(jnp.abs(value) * scale))
        level = jnp.minimum(root * LEVELS + 0.5, LEVELS).astype(I32)
        level = jnp.where(value < 0, -level, level).astype(jnp.int16)
        out_ref[:, l * COLS : (l + 2) * COLS] = level


def first_kernel(where_ref, recv_ref, acc_ref, peak_ref):
    acc_ref[...] = jnp.zeros_like(acc_ref)
    peak = add_sources(where_ref[0], recv_ref, acc_ref)
    peak_ref[...] = jnp.broadcast_to(peak, peak_ref.shape)


def second_kernel(where_ref, recv_ref, given_ref, given_peak_ref, acc_ref, peak_ref):
    acc_ref[...] = given_ref[...]
    peak = add_sources(where_ref[0], recv_ref, acc_ref)
    peak_ref[...] = jnp.maximum(given_peak_ref[...], peak)


def last_kernel(where_ref, least_ref, recv_ref, given_ref, given_peak_ref, prior_ref, out_ref, peak_ref, acc_ref):
    acc_ref[...] = given_ref[...]
    peak = jnp.maximum(given_peak_ref[...], add_sources(where_ref[0], recv_ref, acc_ref))
    peak = jnp.maximum(jnp.max(peak), least_ref[0])
    peak_ref[0] = peak
    finish(where_ref, acc_ref, 1.0 / peak, prior_ref, out_ref)


def finish_kernel(where_ref, peak_ref, acc_ref, prior_ref, out_ref):
    finish(where_ref, acc_ref, 1.0 / peak_ref[0], prior_ref, out_ref)


def sums_cost(recv, high_size):
    sources, height, _ = recv.shape
    rows = (height - CODE_ROWS) // COLS * LANES * sources
    flops = 2 * rows * (LOW * COLS + CODE_ROWS) * high_size
    return pl.CostEstimate(flops=flops, bytes_accessed=recv.size * 2, transcendentals=0)


def sums_of(recv, where, given, high_size):
    shapes = (
        jax.ShapeDtypeStruct((LOW * COLS + CODE_ROWS, high_size), F32),
        jax.ShapeDtypeStruct((8, LANES), F32),
    )
    return pl.pallas_call(
        first_kernel if given is None else second_kernel,
        out_shape=shapes,
        in_specs=[SMEM, VMEM] + ([] if given is None else [VMEM, VMEM]),
        out_specs=(VMEM, VMEM),
        cost_estimate=sums_cost(recv, high_size),
        compiler_params=pltpu.CompilerParams(vmem_limit_bytes=SMALL_VMEM),
        name="sums_first" if given is None else "sums_second",
    )(where, recv, *(given or ()))


def unit_shape(high_size):
    return jax.ShapeDtypeStruct((high_size, LOW * COLS), jnp.int16)


def last_sums(recv, where, given, least, prior, high_size):
    return pl.pallas_call(
        last_kernel,
        out_shape=(unit_shape(high_size), jax.ShapeDtypeStruct((1,), F32)),
        in_specs=[SMEM, SMEM, VMEM, VMEM, VMEM, VMEM],
        out_specs=(VMEM, SMEM),
        scratch_shapes=[pltpu.VMEM(given[0].shape, F32)],
        cost_estimate=sums_cost(recv, high_size),
        compiler_params=pltpu.CompilerParams(vmem_limit_bytes=SMALL_VMEM),
        name="sums_last",
    )(where, least, recv, *given, prior)


def finished(acc, peak, prior, where):
    return pl.pallas_call(
        finish_kernel,
        out_shape=unit_shape(acc.shape[1]),
        in_specs=[SMEM, SMEM, VMEM, VMEM],
        out_specs=VMEM,
        name="finish",
    )(where, peak, acc, prior)


def spread_kernel(counts, where_ref, peak_ref, *refs):
    out_ref = refs[-1]
    first = where_ref[1] == 0
    high_size = out_ref.shape[0] // LOW

    def emit(mine_ref, other_refs):
        at = 0
        for other_ref in other_refs:
            rows = other_ref.shape[0]
            lower = lax.broadcasted_iota(jnp.int16, (rows, LANES), 1) < HALF
            for l in range(0, LOW, 2):
                lanes = slice(l * COLS, (l + 2) * COLS)
                mine, other = mine_ref[at : at + rows, lanes], other_ref[:, lanes]
                left, right = jnp.where(first, mine, other), jnp.where(first, other, mine)
                both = (
                    jnp.where(lower, left, pltpu.roll(right, HALF, 1)),
                    jnp.where(lower, pltpu.roll(left, HALF, 1), right),
                )
                for k, level in enumerate(both):
                    t = level.astype(I32).astype(F32) * (1.0 / LEVELS)
                    s = t * jnp.abs(t)
                    start = (l + k) * high_size + at
                    out_ref[start : start + rows, :] = s * jnp.abs(s) * peak_ref[0]
            at += rows

    at = 0
    for p, count in enumerate(counts):
        pl.when(pl.program_id(0) == p)(functools.partial(emit, refs[at], refs[at + 1 : at + 1 + count]))
        at += 1 + count


def spread(first, pairs, where, peak, width, into):
    high_size = pairs[0][0].shape[0]
    total = LOW * high_size
    pieces = [p for mine, others in pairs for p in (mine, *others)]
    extra = [] if into is None else [into]
    return pl.pallas_call(
        functools.partial(spread_kernel, tuple(len(others) for _, others in pairs)),
        grid_spec=pltpu.PrefetchScalarGridSpec(
            num_scalar_prefetch=1,
            grid=(len(pairs),),
            in_specs=[SMEM] + [VMEM for _ in pieces] + [pl.BlockSpec(memory_space=pl.ANY) for _ in extra],
            out_specs=pl.BlockSpec((total, LANES), lambda p, w: (0, w[2 + first + p])),
        ),
        out_shape=jax.ShapeDtypeStruct((total, width), F32),
        input_output_aliases={2 + len(pieces): 0} if extra else {},
        cost_estimate=pl.CostEstimate(
            flops=8 * len(pairs) * total * LANES,
            bytes_accessed=6 * len(pairs) * total * LANES,
            transcendentals=0,
        ),
        compiler_params=pltpu.CompilerParams(vmem_limit_bytes=SMALL_VMEM),
        name="spread",
    )(where, peak, *pieces, *extra)


def z_shifts(nz):
    return [0, 1, nz - 1] + list(range(2, nz - 1))


def gather(unit, peak, where, width):
    nz = lax.axis_size("z")
    assert nz == 4
    half = unit.shape[0] // 2

    def send(piece, axis, shift=1):
        size = lax.axis_size(axis)
        return lax.ppermute(piece, axis, [(i, (i + shift) % size) for i in range(size)])

    shifts = z_shifts(nz)
    held = [unit] + [send(unit, "z", shifts[n]) for n in range(1, nz)]
    from_x = [send(piece, "x") for piece in held]
    from_y = [send(piece, "y") for piece in held]
    near = send(from_y[0], "x")
    diagonal = [
        [near],
        [send(from_x[1], "y")],
        [send(from_y[2][:half], "x"), send(from_x[2][half:], "y")],
        [send(near, "z", shifts[3])],
    ]
    pairs = [(from_y[n], diagonal[n]) if m else (held[n], [from_x[n]]) for n, m in PAIRS]
    out = None
    for start, end in SPREADS:
        out = spread(start, pairs[start:end], where, peak, width, out)
    return out


def nearest(points, point_sq, part):
    inner = lax.dot_general(points, part, (((1,), (1,)), ((), ())), preferred_element_type=F32)
    part_f = part.astype(F32)
    part_sq = jnp.sum(part_f * part_f, axis=1)
    return jnp.min(point_sq[:, None] - 2.0 * inner + part_sq[None, :], axis=1)


def shards(points, centroids, assign, keep_mask):
    width = points.shape[1]
    shard_rows = centroids.shape[0]
    high_size = shard_rows // LOW
    z, y, x = (lax.axis_index(a) for a in OWNERS)
    nz, ny, nx = (lax.axis_size(a) for a in OWNERS)
    assert nx == 2 and ny == 2 and nz * ny * nx * COLS == width
    block = z * ny + y
    shifts = z_shifts(nz)
    columns = [((z - shifts[n]) % nz) * ny + (y ^ m) for n, m in PAIRS]
    where = jnp.stack([lax.axis_index("mp") * shard_rows, x, *columns]).astype(I32)

    parcels, centroids = lax.optimization_barrier((pack(points, assign, keep_mask), centroids))
    recv = lax.all_to_all(parcels, OWNERS, 0, 0, tiled=True)
    others = lax.ppermute(centroids, "mp", SWAP)

    point_f = points.astype(F32)
    point_sq = jnp.sum(point_f * point_f, axis=1)
    best = jnp.minimum(nearest(points, point_sq, centroids), nearest(points, point_sq, others)) / width
    least = jnp.maximum(jnp.max(jnp.abs(centroids)).astype(F32), TINY)[None]
    prior = lax.dynamic_slice_in_dim(centroids, block * LANES, LANES, 1)
    recv, best, least, prior, where = lax.optimization_barrier((recv, best, least, prior, where))

    partner = lax.ppermute(recv, "mp", SWAP)
    given = sums_of(recv, where, None, high_size)
    if lax.axis_size("g") > 1:
        acc, peak = sums_of(partner, where, given, high_size)
        acc, peak = lax.psum(acc, "g"), lax.pmax(jnp.max(peak), "g")
        peak = jnp.maximum(peak, least)
        unit = finished(acc, peak, prior, where)
    else:
        unit, peak = last_sums(partner, where, given, least, prior, high_size)

    out = gather(unit, peak, where, width)
    return out, best


def split_dp(mesh, width):
    dp, mp = mesh.shape["dp"], mesh.shape["mp"]
    owners = width // COLS
    devices = mesh.devices.reshape(dp // owners, owners // 4, 2, 2, mp)
    return Mesh(devices, AXES)


def solution(mesh):
    rows = P(AXES)

    def step(points, centroids, assign, keep_mask):
        return jax.shard_map(
            shards,
            mesh=split_dp(mesh, points.shape[1]),
            in_specs=(P(AXES, None), P("mp", None), rows, rows),
            out_specs=(P("mp", None), rows),
            check_vma=False,
        )(points, centroids, assign, keep_mask)

    return step
```

```python
import functools

import jax
import jax.numpy as jnp
from jax import lax
from jax.experimental import pallas as pl
from jax.experimental.pallas import tpu as pltpu
from jax.sharding import Mesh, PartitionSpec as P


LANES = 128
COLS = 64
LOW = 4
DIGIT = 7
CODE_ROWS = 16
LEVELS = 32767.0
TINY = 1e-30
GROUP = 16
SMALL_VMEM = 24 << 20
F32, BF16, I32 = jnp.float32, jnp.bfloat16, jnp.int32
HALF = LANES // 2
SWAP = [(0, 1), (1, 0)]
OWNERS = ("z", "y", "x")
AXES = ("g",) + OWNERS + ("mp",)

PAIRS = ((0, 0), (0, 1), (1, 0), (2, 0), (1, 1), (3, 0), (3, 1), (2, 1))
SPREADS = ((0, 2), (2, 4), (4, 6), (6, 8))
VMEM = pl.BlockSpec(memory_space=pltpu.VMEM)
SMEM = pl.BlockSpec(memory_space=pltpu.SMEM)


def pack_kernel(points_ref, assign_ref, keep_ref, out_ref):
    rows, width = points_ref.shape
    blocks = rows // LANES
    kept = keep_ref[...]
    assign = assign_ref[...]
    high = jnp.where(kept > 0, assign >> DIGIT, -1).astype(F32)
    low = (assign & ((1 << DIGIT) - 1)).astype(F32)
    weight = kept.astype(F32)
    peak = jnp.zeros((1, LANES), F32)
    for b in range(blocks):
        for c in range(width // LANES):
            tile = points_ref[b * LANES : (b + 1) * LANES, c * LANES : (c + 1) * LANES].T
            out_ref[2 * c, b * COLS : (b + 1) * COLS, :] = tile[:COLS]
            out_ref[2 * c + 1, b * COLS : (b + 1) * COLS, :] = tile[COLS:]
            size = jnp.max(jnp.abs(tile.astype(F32)), axis=0, keepdims=True)
            peak = jnp.maximum(peak, size * weight[b : b + 1])
    pad = jnp.zeros((CODE_ROWS - 2 * blocks - 1, LANES), F32)
    codes = jnp.concatenate([high, low, peak, pad], axis=0).astype(BF16)
    for s in range(out_ref.shape[0]):
        out_ref[s, blocks * COLS :, :] = codes


def pack(points, assign, keep):
    rows, width = points.shape
    blocks = rows // LANES
    assert 2 * blocks + 1 <= CODE_ROWS
    shape = (width // COLS, blocks * COLS + CODE_ROWS, LANES)
    return pl.pallas_call(
        pack_kernel,
        out_shape=jax.ShapeDtypeStruct(shape, BF16),
        in_specs=[VMEM] * 3,
        out_specs=VMEM,
        cost_estimate=pl.CostEstimate(
            flops=2 * rows * width, bytes_accessed=4 * rows * width, transcendentals=0
        ),
        name="pack",
    )(points, assign.reshape(blocks, LANES), keep.reshape(blocks, LANES))


def add_sources(base, recv_ref, acc_ref):
    sources, height, _ = recv_ref.shape
    high_size = acc_ref.shape[1]
    blocks = (height - CODE_ROWS) // COLS
    rows = blocks * LANES
    shift = high_size.bit_length() - 1

    group = min(GROUP, sources)

    def factors(s):
        codes = recv_ref[s, blocks * COLS :, :].astype(F32)
        local = (codes[:blocks] * float(1 << DIGIT) + codes[blocks : 2 * blocks]).astype(I32) - base
        local = jnp.concatenate([local[b : b + 1] for b in range(blocks)], axis=1)
        k_low, k_high = local >> shift, local & (high_size - 1)
        hot = (lax.broadcasted_iota(I32, (high_size, rows), 0) == k_high).astype(F32).astype(BF16)
        data = [recv_ref[s, b * COLS : (b + 1) * COLS, :] for b in range(blocks)]
        data = jnp.concatenate(data, axis=1)
        masks = [(k_low == l).astype(F32) for l in range(LOW)]
        parts = [data * m.astype(BF16) for m in masks]
        pad = jnp.zeros((CODE_ROWS - LOW, rows), F32)
        parts.append(jnp.concatenate(masks + [pad], axis=0).astype(BF16))
        return jnp.concatenate(parts, axis=0), hot, codes[2 * blocks : 2 * blocks + 1]

    def step(i, peak):
        left, hot, size = zip(*[factors(i * group + u) for u in range(group)])
        left, hot = jnp.concatenate(left, axis=1), jnp.concatenate(hot, axis=1)
        acc_ref[...] += lax.dot_general(
            left, hot, (((1,), (1,)), ((), ())), preferred_element_type=F32
        )
        return functools.reduce(jnp.maximum, size, peak)

    return lax.fori_loop(0, sources // group, step, jnp.zeros((1, LANES), F32))


def finish(where_ref, acc_ref, scale, prior_ref, out_ref):
    high_size = acc_ref.shape[1]
    counts = acc_ref[LOW * COLS : LOW * COLS + 8, :]
    inverse = 1.0 / jnp.maximum(counts, 1.0)
    tall = counts.T
    odd = where_ref[1] > 0
    lower = lax.broadcasted_iota(I32, (high_size, LANES), 1) < HALF
    for l in range(0, LOW, 2):
        mean = [acc_ref[k * COLS : (k + 1) * COLS, :] * inverse[k : k + 1] for k in (l, l + 1)]
        mean = jnp.concatenate(mean, axis=0).T
        priors = [prior_ref[k * high_size : (k + 1) * high_size, :].astype(F32) for k in (l, l + 1)]
        turned = [pltpu.roll(p, HALF, 1) for p in priors]
        prior = jnp.where(
            lower, jnp.where(odd, turned[0], priors[0]), jnp.where(odd, priors[1], turned[1])
        )
        count = jnp.where(lower, tall[:, l : l + 1], tall[:, l + 1 : l + 2])
        value = jnp.where(count > 0.5, mean, prior)
        root = jnp.sqrt(jnp.sqrt(jnp.abs(value) * scale))
        level = jnp.minimum(root * LEVELS + 0.5, LEVELS).astype(I32)
        level = jnp.where(value < 0, -level, level).astype(jnp.int16)
        out_ref[:, l * COLS : (l + 2) * COLS] = level


def first_kernel(where_ref, recv_ref, acc_ref, peak_ref):
    acc_ref[...] = jnp.zeros_like(acc_ref)
    peak = add_sources(where_ref[0], recv_ref, acc_ref)
    peak_ref[...] = jnp.broadcast_to(peak, peak_ref.shape)


def second_kernel(where_ref, recv_ref, given_ref, given_peak_ref, acc_ref, peak_ref):
    acc_ref[...] = given_ref[...]
    peak = add_sources(where_ref[0], recv_ref, acc_ref)
    peak_ref[...] = jnp.maximum(given_peak_ref[...], peak)


def last_kernel(where_ref, least_ref, recv_ref, given_ref, given_peak_ref, prior_ref, out_ref, peak_ref, acc_ref):
    acc_ref[...] = given_ref[...]
    peak = jnp.maximum(given_peak_ref[...], add_sources(where_ref[0], recv_ref, acc_ref))
    peak = jnp.maximum(jnp.max(peak), least_ref[0])
    peak_ref[0] = peak
    finish(where_ref, acc_ref, 1.0 / peak, prior_ref, out_ref)


def finish_kernel(where_ref, peak_ref, acc_ref, prior_ref, out_ref):
    finish(where_ref, acc_ref, 1.0 / peak_ref[0], prior_ref, out_ref)


def sums_cost(recv, high_size):
    sources, height, _ = recv.shape
    rows = (height - CODE_ROWS) // COLS * LANES * sources
    flops = 2 * rows * (LOW * COLS + CODE_ROWS) * high_size
    return pl.CostEstimate(flops=flops, bytes_accessed=recv.size * 2, transcendentals=0)


def sums_of(recv, where, given, high_size):
    shapes = (
        jax.ShapeDtypeStruct((LOW * COLS + CODE_ROWS, high_size), F32),
        jax.ShapeDtypeStruct((8, LANES), F32),
    )
    return pl.pallas_call(
        first_kernel if given is None else second_kernel,
        out_shape=shapes,
        in_specs=[SMEM, VMEM] + ([] if given is None else [VMEM, VMEM]),
        out_specs=(VMEM, VMEM),
        cost_estimate=sums_cost(recv, high_size),
        compiler_params=pltpu.CompilerParams(vmem_limit_bytes=SMALL_VMEM),
        name="sums_first" if given is None else "sums_second",
    )(where, recv, *(given or ()))


def unit_shape(high_size):
    return jax.ShapeDtypeStruct((high_size, LOW * COLS), jnp.int16)


def last_sums(recv, where, given, least, prior, high_size):
    return pl.pallas_call(
        last_kernel,
        out_shape=(unit_shape(high_size), jax.ShapeDtypeStruct((1,), F32)),
        in_specs=[SMEM, SMEM, VMEM, VMEM, VMEM, VMEM],
        out_specs=(VMEM, SMEM),
        scratch_shapes=[pltpu.VMEM(given[0].shape, F32)],
        cost_estimate=sums_cost(recv, high_size),
        compiler_params=pltpu.CompilerParams(vmem_limit_bytes=SMALL_VMEM),
        name="sums_last",
    )(where, least, recv, *given, prior)


def finished(acc, peak, prior, where):
    return pl.pallas_call(
        finish_kernel,
        out_shape=unit_shape(acc.shape[1]),
        in_specs=[SMEM, SMEM, VMEM, VMEM],
        out_specs=VMEM,
        name="finish",
    )(where, peak, acc, prior)


def spread_kernel(counts, where_ref, peak_ref, *refs):
    out_ref = refs[-1]
    first = where_ref[1] == 0
    high_size = out_ref.shape[0] // LOW

    def emit(mine_ref, other_refs):
        at = 0
        for other_ref in other_refs:
            rows = other_ref.shape[0]
            lower = lax.broadcasted_iota(jnp.int16, (rows, LANES), 1) < HALF
            for l in range(0, LOW, 2):
                lanes = slice(l * COLS, (l + 2) * COLS)
                mine, other = mine_ref[at : at + rows, lanes], other_ref[:, lanes]
                left, right = jnp.where(first, mine, other), jnp.where(first, other, mine)
                both = (
                    jnp.where(lower, left, pltpu.roll(right, HALF, 1)),
                    jnp.where(lower, pltpu.roll(left, HALF, 1), right),
                )
                for k, level in enumerate(both):
                    t = level.astype(I32).astype(F32) * (1.0 / LEVELS)
                    s = t * jnp.abs(t)
                    start = (l + k) * high_size + at
                    out_ref[start : start + rows, :] = s * jnp.abs(s) * peak_ref[0]
            at += rows

    at = 0
    for p, count in enumerate(counts):
        pl.when(pl.program_id(0) == p)(functools.partial(emit, refs[at], refs[at + 1 : at + 1 + count]))
        at += 1 + count


def spread(first, pairs, where, peak, width, into):
    high_size = pairs[0][0].shape[0]
    total = LOW * high_size
    pieces = [p for mine, others in pairs for p in (mine, *others)]
    extra = [] if into is None else [into]
    return pl.pallas_call(
        functools.partial(spread_kernel, tuple(len(others) for _, others in pairs)),
        grid_spec=pltpu.PrefetchScalarGridSpec(
            num_scalar_prefetch=1,
            grid=(len(pairs),),
            in_specs=[SMEM] + [VMEM for _ in pieces] + [pl.BlockSpec(memory_space=pl.ANY) for _ in extra],
            out_specs=pl.BlockSpec((total, LANES), lambda p, w: (0, w[2 + first + p])),
        ),
        out_shape=jax.ShapeDtypeStruct((total, width), F32),
        input_output_aliases={2 + len(pieces): 0} if extra else {},
        cost_estimate=pl.CostEstimate(
            flops=8 * len(pairs) * total * LANES,
            bytes_accessed=6 * len(pairs) * total * LANES,
            transcendentals=0,
        ),
        compiler_params=pltpu.CompilerParams(vmem_limit_bytes=SMALL_VMEM),
        name="spread",
    )(where, peak, *pieces, *extra)


def z_shifts(nz):
    return [0, 1, nz - 1] + list(range(2, nz - 1))


def gather(unit, peak, where, width):
    nz = lax.axis_size("z")
    assert nz == 4
    half = unit.shape[0] // 2

    def send(piece, axis, shift=1):
        size = lax.axis_size(axis)
        return lax.ppermute(piece, axis, [(i, (i + shift) % size) for i in range(size)])

    shifts = z_shifts(nz)
    held = [unit] + [send(unit, "z", shifts[n]) for n in range(1, nz)]
    from_x = [send(piece, "x") for piece in held]
    from_y = [send(piece, "y") for piece in held]
    near = send(from_y[0], "x")
    diagonal = [
        [near],
        [send(from_x[1], "y")],
        [send(from_y[2][:half], "x"), send(from_x[2][half:], "y")],
        [send(near, "z", shifts[3])],
    ]
    pairs = [(from_y[n], diagonal[n]) if m else (held[n], [from_x[n]]) for n, m in PAIRS]
    out = None
    for start, end in SPREADS:
        out = spread(start, pairs[start:end], where, peak, width, out)
    return out


def nearest(points, point_sq, part):
    inner = lax.dot_general(points, part, (((1,), (1,)), ((), ())), preferred_element_type=F32)
    part_f = part.astype(F32)
    part_sq = jnp.sum(part_f * part_f, axis=1)
    return jnp.min(point_sq[:, None] - 2.0 * inner + part_sq[None, :], axis=1)


def shards(points, centroids, assign, keep_mask):
    width = points.shape[1]
    shard_rows = centroids.shape[0]
    high_size = shard_rows // LOW
    z, y, x = (lax.axis_index(a) for a in OWNERS)
    nz, ny, nx = (lax.axis_size(a) for a in OWNERS)
    assert nx == 2 and ny == 2 and nz * ny * nx * COLS == width
    block = z * ny + y
    shifts = z_shifts(nz)
    columns = [((z - shifts[n]) % nz) * ny + (y ^ m) for n, m in PAIRS]
    where = jnp.stack([lax.axis_index("mp") * shard_rows, x, *columns]).astype(I32)

    parcels, centroids = lax.optimization_barrier((pack(points, assign, keep_mask), centroids))
    recv = lax.all_to_all(parcels, OWNERS, 0, 0, tiled=True)
    others = lax.ppermute(centroids, "mp", SWAP)

    point_f = points.astype(F32)
    point_sq = jnp.sum(point_f * point_f, axis=1)
    best = jnp.minimum(nearest(points, point_sq, centroids), nearest(points, point_sq, others)) / width
    least = jnp.maximum(jnp.max(jnp.abs(centroids)).astype(F32), TINY)[None]
    prior = lax.dynamic_slice_in_dim(centroids, block * LANES, LANES, 1)
    recv, best, least, prior, where = lax.optimization_barrier((recv, best, least, prior, where))

    partner = lax.ppermute(recv, "mp", SWAP)
    given = sums_of(recv, where, None, high_size)
    if lax.axis_size("g") > 1:
        acc, peak = sums_of(partner, where, given, high_size)
        acc, peak = lax.psum(acc, "g"), lax.pmax(jnp.max(peak), "g")
        peak = jnp.maximum(peak, least)
        unit = finished(acc, peak, prior, where)
    else:
        unit, peak = last_sums(partner, where, given, least, prior, high_size)

    out = gather(unit, peak, where, width)
    return out, best


def split_dp(mesh, width):
    dp, mp = mesh.shape["dp"], mesh.shape["mp"]
    owners = width // COLS
    devices = mesh.devices.reshape(dp // owners, owners // 4, 2, 2, mp)
    return Mesh(devices, AXES)


def solution(mesh):
    rows = P(AXES)

    def step(points, centroids, assign, keep_mask):
        return jax.shard_map(
            shards,
            mesh=split_dp(mesh, points.shape[1]),
            in_specs=(P(AXES, None), P("mp", None), rows, rows),
            out_specs=(P("mp", None), rows),
            check_vma=False,
        )(points, centroids, assign, keep_mask)

    return step
```
